32 devices in a mesh: grp: 2 (over x), col: 8 (over z, core), lay: 2 (over y).
Axes of the slice: x: 2, y: 2, z: 4, core: 2. Of those that a mesh axis runs over, the one named last changes fastest.
Arguments:
- gradient: float32 [2, 2, 24, 6144, 128], P('grp', 'lay', None, 'col'), may hold values from -410 to 410
- momentum: float32 [2, 2, 24, 6144, 128], P('grp', 'lay', None, 'col'), may hold values from -820 to 820
- probe_vector: float32 [128], replicated, may hold values from -4 to 4
Outputs:
- new_momentum: float32 [2, 2, 24, 6144, 128], P('grp', 'lay', None, 'col')
- update: float32 [2, 2, 24, 6144, 128], P('grp', 'lay', None, 'col')
The draws below stay inside these ranges and needn't reach their ends.
All inputs are finite; a program needn't handle non-finite values.
Results may differ from the reference program's by a relative error of at most 0.00022.
Values sent between devices are 32-bit elements; how exact they have to be, the bound alone decides.
No kernel may reach another device: no remote copies, remote signals or barrier semaphores. Data moves between devices by JAX's collectives and lax.ppermute only.
A program may use at most 128 MiB of HBM per device.

```python
import math
import jax
import jax.numpy as jnp
from jax import lax

D = 6144
HEAD_SIZE = 128
HEADS = 24
ITERS = 3
GROUPS = 2
LAYERS = 2


def shared_scale(key):
    base_key = jax.random.fold_in(key, 7)
    count = GROUPS * LAYERS
    position = jnp.arange(count, dtype=jnp.float32) / max(count - 1, 1)
    rising = jnp.exp(position * jnp.log(3.0))
    row_low, row_high = (0.5, 2.0)
    jitter = jnp.exp(jax.random.uniform(jax.random.fold_in(base_key, 1), (count, HEADS), jnp.float32, jnp.log(0.5), jnp.log(2.0)))
    per_block = (rising[:, None] * jitter).reshape((GROUPS, LAYERS, HEADS, 1, 1))
    row_scale = jnp.exp(jax.random.uniform(jax.random.fold_in(base_key, 2), (GROUPS, LAYERS, HEADS, 1, HEAD_SIZE), jnp.float32, jnp.log(row_low), jnp.log(row_high)))
    return per_block * row_scale


def noise_field(key, salt):
    shape = (GROUPS, LAYERS, HEADS, D, HEAD_SIZE)
    noise = jax.random.truncated_normal(jax.random.fold_in(key, salt), -4.0, 4.0, shape, jnp.float32)
    return noise


def draw_gradient(key, part):
    return (noise_field(key, 11) * shared_scale(key)).astype(jnp.float32)


def draw_momentum(key, part):
    return (2.0 * noise_field(key, 21) * shared_scale(key)).astype(jnp.float32)


def scatter_about(stream_key, dims, scale, limit, held_as=jnp.bfloat16):
    entries = jax.random.normal(stream_key, dims, jnp.float32) * scale
    return jnp.minimum(jnp.maximum(entries, -limit), limit).astype(held_as)


def setup_inputs(seed: int = 0) -> dict:
    arg_keys = jax.random.split(jax.random.key(seed), 4)
    return {
        "gradient": draw_gradient(jax.random.fold_in(arg_keys[3], 71), 0),
        "momentum": draw_momentum(jax.random.fold_in(arg_keys[3], 71), 0),
        "probe_vector": scatter_about(arg_keys[2], (HEAD_SIZE,), 1.0, 4.0, jnp.float32),
    }


MOMENTUM_DECAY = 0.95
LINEAR_TERM = 3.4445
CUBIC_TERM = -4.775
QUINTIC_TERM = 2.0315
EPSILON = 1e-06
PRECISE = lax.Precision.HIGHEST

def reference(gradient, momentum, probe_vector):
    new_momentum = MOMENTUM_DECAY * momentum + gradient
    blend = gradient + MOMENTUM_DECAY * new_momentum
    probe_norm = jnp.sqrt(jnp.sum(probe_vector * probe_vector) + EPSILON)

    def estimate_one(matrix):
        gram_matrix = jnp.dot(matrix.T, matrix, preferred_element_type=jnp.float32, precision=PRECISE)
        product = jnp.dot(gram_matrix, probe_vector, preferred_element_type=jnp.float32, precision=PRECISE)
        return jnp.sqrt(jnp.sum(product * product) + EPSILON) / probe_norm
    stacked = blend.reshape((-1, D, HEAD_SIZE))
    estimate = lax.map(estimate_one, stacked).reshape((GROUPS, LAYERS, HEADS))
    bound_value = 2.0 * jnp.sqrt(lax.optimization_barrier(jnp.max(estimate, axis=(0, 1))))
    scaled = blend / bound_value[None, None, :, None, None]

    def polish(matrix):
        identity = jnp.eye(HEAD_SIZE, dtype=matrix.dtype)
        for counter in range(ITERS):
            gram_matrix = jnp.dot(matrix.T, matrix, preferred_element_type=jnp.float32, precision=PRECISE)
            square = jnp.dot(gram_matrix, gram_matrix, preferred_element_type=jnp.float32, precision=PRECISE)
            mixing = LINEAR_TERM * identity + CUBIC_TERM * gram_matrix + QUINTIC_TERM * square
            matrix = jnp.dot(matrix, mixing, preferred_element_type=jnp.float32, precision=PRECISE)
        return matrix
    polished = lax.map(polish, scaled.reshape((-1, D, HEAD_SIZE))).reshape(blend.shape)
    update = polished * (0.2 * math.sqrt(D))
    return (new_momentum, update)
```

```python
import functools
import math

import jax
import jax.numpy as jnp
from jax import lax
from jax.experimental import pallas as pl
from jax.experimental.pallas import tpu as pltpu
from jax.sharding import PartitionSpec as P


ITERS = 3


MOMENTUM_DECAY = 0.95
LINEAR_TERM = 3.4445
CUBIC_TERM = -4.775
QUINTIC_TERM = 2.0315
EPSILON = 1e-06
PRECISE = lax.Precision.HIGHEST


def summed_gram(stack):
    partial_gram = jnp.einsum("glhdr,glhds->glhrs", stack, stack, precision=PRECISE)
    return lax.psum(partial_gram, "col")


def head_bound(product, probe_norm):
    estimate = jnp.sqrt(jnp.sum(product * product, axis=-1) + EPSILON) / probe_norm
    local_most = jnp.max(estimate, axis=(0, 1))
    overall = lax.pmax(local_most, ("grp", "lay"))
    return 2.0 * jnp.sqrt(overall)


def on_device_general(gradient, momentum, probe_vector):
    new_momentum = MOMENTUM_DECAY * momentum + gradient
    blend = gradient + MOMENTUM_DECAY * new_momentum
    width = blend.shape[-1]
    probe_norm = jnp.sqrt(jnp.sum(probe_vector * probe_vector) + EPSILON)
    raw_gram = summed_gram(blend)
    product = jnp.einsum("glhrs,s->glhr", raw_gram, probe_vector, precision=PRECISE)
    bound_value = head_bound(product, probe_norm)
    scaled = blend / bound_value[None, None, :, None, None]
    current = raw_gram / (bound_value * bound_value)[None, None, :, None, None]
    identity = jnp.eye(width, dtype=jnp.float32)
    total = jnp.broadcast_to(identity, current.shape)
    for counter in range(ITERS):
        square = jnp.einsum("glhrs,glhst->glhrt", current, current, precision=PRECISE)
        mixing = LINEAR_TERM * identity + CUBIC_TERM * current + QUINTIC_TERM * square
        total = jnp.einsum("glhrs,glhst->glhrt", total, mixing, precision=PRECISE)
        if counter + 1 < ITERS:
            halfway = jnp.einsum("glhrs,glhst->glhrt", mixing, current, precision=PRECISE)
            current = jnp.einsum("glhrs,glhst->glhrt", halfway, mixing, precision=PRECISE)
    polished = jnp.einsum("glhdr,glhrs->glhds", scaled, total, precision=PRECISE)
    update = polished * (0.2 * math.sqrt(blend.shape[3] * lax.psum(1, "col")))
    return (new_momentum, update)


F32 = jnp.float32
BF16 = jnp.bfloat16
VMEM_LIMIT = 60 * 2**20
ROOMY = 48 * 2**20


def iotas(shape):
    return lax.broadcasted_iota(jnp.int32, shape, 0), lax.broadcasted_iota(jnp.int32, shape, 1)


def packed_rows(heads, width):
    full, odd = divmod(heads, 2)
    return full * width + odd * (width // 2) + 8 * (full + odd)


def pack(mats):
    width = mats[0].shape[0]
    row, col = iotas((width, width))
    rows8, _ = iotas((8, width))
    body, diags = [], []
    for i in range(0, len(mats) - 1, 2):
        first, second = mats[i], mats[i + 1]
        body.append(jnp.where(row >= col, first, second))
        diag = jnp.sum(jnp.where(row == col, second, 0.0), axis=0, keepdims=True)
        diags.append(jnp.where(rows8 == 0, diag, 0.0))
    if len(mats) % 2:
        half = width // 2
        last = mats[-1]
        row, col = iotas((half, width))
        rolled = pltpu.roll(last[half:], half, 1)
        body.append(jnp.where((col < half) & (col > row), rolled, last[:half]))
        diag = jnp.sum(jnp.where(row == col, rolled, 0.0), axis=0, keepdims=True)
        diags.append(jnp.where(rows8 == 0, diag, 0.0))
    return body + diags


def store_packed(ref, mats):
    start = 0
    for piece in pack(mats):
        ref[start : start + piece.shape[0]] = piece
        start += piece.shape[0]


def unpack(value, heads):
    width = value.shape[1]
    half = width // 2
    full, odd = divmod(heads, 2)
    diag_start = full * width + odd * half
    row, col = iotas((width, width))
    mats = []
    for i in range(full):
        square = value[i * width : (i + 1) * width]
        turned = square.T
        diag = value[diag_start + 8 * i : diag_start + 8 * i + 1]
        mats.append(jnp.where(row >= col, square, turned))
        mats.append(jnp.where(row < col, square, jnp.where(row > col, turned, diag)))
    if odd:
        top = value[full * width : full * width + half]
        turned = jnp.concatenate([top, jnp.zeros_like(top)], axis=0).T
        diag = value[diag_start + 8 * full : diag_start + 8 * full + 1]
        row, col = iotas((half, width))
        upper = jnp.where((col < half) & (row < col), turned[:half], top)
        corner = jnp.where(row < col, top, jnp.where(row > col, turned[:half], diag))
        lower = jnp.where(col < half, turned[half:], pltpu.roll(corner, half, 1))
        mats.append(jnp.concatenate([upper, lower], axis=0))
    return mats


def split(value):
    high = value.astype(BF16)
    return high, (value - high.astype(F32)).astype(BF16)


def head_specs(per, shape):
    return [pl.BlockSpec((1,) + shape, lambda j, ids, i=i: (ids[j] * per + i, 0, 0)) for i in range(per)]


def gram_kernel(per, group_ref, *refs):
    del group_ref
    gradient_refs, momentum_refs, refs = refs[:per], refs[per : 2 * per], refs[2 * per :]
    mats = []
    for gradient_ref, momentum_ref in zip(gradient_refs, momentum_refs):
        gradient = gradient_ref[0]
        blend = gradient + MOMENTUM_DECAY * (MOMENTUM_DECAY * momentum_ref[0] + gradient)
        high, low = split(blend)
        both = jnp.concatenate([high, low], axis=1)
        product = lax.dot_general(high, both, (((0,), (0,)), ((), ())), preferred_element_type=F32)
        width = blend.shape[1]
        cross = product[:, width:]
        mats.append(product[:, :width] + (cross + cross.T))
    if len(refs) == 1:
        store_packed(refs[0].at[0], mats)
        return
    other_ref, *out_refs, held_ref = refs
    store_packed(held_ref, mats)
    for k, out_ref in enumerate(out_refs):

        @pl.when(pl.program_id(0) == k)
        def _(out_ref=out_ref):
            out_ref[...] = held_ref[...] + other_ref[0]


def local_grams(groups, gradient, momentum, per, other=None):
    _, rows, width = gradient.shape
    count = groups.shape[0]
    blocks = head_specs(per, (rows, width))
    packed = packed_rows(per, width)
    piece = pl.BlockSpec((1, packed, width), lambda j, ids: (j, 0, 0))
    operands, in_specs = [groups] + [gradient] * per + [momentum] * per, blocks + blocks
    if other is None:
        out_shape = jax.ShapeDtypeStruct((count, packed, width), F32)
        out_specs, scratch = piece, []
    else:
        operands.append(other)
        in_specs.append(piece)
        out_shape = [jax.ShapeDtypeStruct((packed, width), F32)] * count
        out_specs = [pl.BlockSpec((packed, width), lambda j, ids: (0, 0))] * count
        scratch = [pltpu.VMEM((packed, width), F32)]
    return pl.pallas_call(
        functools.partial(gram_kernel, per),
        name="local_grams",
        out_shape=out_shape,
        grid_spec=pltpu.PrefetchScalarGridSpec(
            num_scalar_prefetch=1,
            grid=(count,),
            in_specs=in_specs,
            out_specs=out_specs,
            scratch_shapes=scratch,
        ),
        cost_estimate=pl.CostEstimate(
            flops=count * per * rows * width * width * 8,
            bytes_accessed=count * per * rows * width * 8,
            transcendentals=0,
        ),
        compiler_params=pltpu.CompilerParams(vmem_limit_bytes=VMEM_LIMIT),
    )(*operands)


def momentum_kernel(per, *refs):
    new_ref, halves_ref = refs[-2:]
    for i in range(per):
        gradient = refs[i][0]
        new = MOMENTUM_DECAY * refs[per + i][0] + gradient
        new_ref[i] = new
        high, low = split(gradient + MOMENTUM_DECAY * new)
        width = gradient.shape[1]
        halves_ref[i, :, :width] = high
        halves_ref[i, :, width:] = low


def update_momentum(gradient, momentum, per, start, stop, partly=()):
    heads, rows, width = gradient.shape
    by_group = lambda j: (j + start, 0, 0)
    block = pl.BlockSpec((per, rows, width), by_group)
    heads_of = [pl.BlockSpec((1, rows, width), lambda j, i=i: ((j + start) * per + i, 0, 0)) for i in range(per)]
    return pl.pallas_call(
        functools.partial(momentum_kernel, per),
        name="update_momentum",
        grid=(stop - start,),
        in_specs=heads_of + heads_of + [pl.BlockSpec(memory_space=pl.ANY)] * len(partly),
        out_specs=[block, pl.BlockSpec((per, rows, 2 * width), by_group)],
        out_shape=[
            jax.ShapeDtypeStruct(gradient.shape, F32),
            jax.ShapeDtypeStruct((heads, rows, 2 * width), BF16),
        ],
        input_output_aliases={2 * per: 0, 2 * per + 1: 1} if partly else {},
        cost_estimate=pl.CostEstimate(
            flops=(stop - start) * per * rows * width * 400,
            bytes_accessed=(stop - start) * per * rows * width * 16,
            transcendentals=0,
        ),
        compiler_params=pltpu.CompilerParams(vmem_limit_bytes=ROOMY),
    )(*[gradient] * per, *[momentum] * per, *partly)


def estimate_kernel(per, probe_ref, *refs):
    *pieces, gram_ref, estimate_ref = refs
    total = pieces[0][...]
    for piece in pieces[1:]:
        total = total + piece[...]
    probe = probe_ref[...]
    probe_norm = jnp.sqrt(jnp.sum(probe * probe, keepdims=True) + EPSILON)
    row, _ = iotas(estimate_ref.shape)
    estimates = jnp.zeros(estimate_ref.shape, F32)
    for i, gram in enumerate(unpack(total, per)):
        gram_ref[i] = gram
        product = jnp.sum(gram * probe, axis=1, keepdims=True)
        estimate = jnp.sqrt(jnp.sum(product * product, keepdims=True) + EPSILON) / probe_norm
        estimates = jnp.where(row == i, estimate, estimates)
    estimate_ref[...] = estimates


def sum_and_estimate(pieces, probe, per):
    width = pieces[0].shape[1]
    return pl.pallas_call(
        functools.partial(estimate_kernel, per),
        name="sum_and_estimate",
        out_shape=[
            jax.ShapeDtypeStruct((per, width, width), F32),
            jax.ShapeDtypeStruct((-(-per // 8) * 8, width), F32),
        ],
    )(probe, *pieces)


def precise_dot(left, right):
    return jnp.dot(left, right, precision=PRECISE, preferred_element_type=F32)


def newton_schulz_kernel(depth, estimate_ref, gram_ref, out_ref):
    per, width = gram_ref.shape[:2]
    row, col = iotas((width, width))
    identity = jnp.where(row == col, 1.0, 0.0)
    bounds = [2.0 * jnp.sqrt(estimate_ref[i : i + 1]) for i in range(per)]
    current = [gram_ref[i] / (bounds[i] * bounds[i]) for i in range(per)]
    total = None
    for counter in range(ITERS):
        square = [precise_dot(a, a) for a in current]
        mixing = [
            LINEAR_TERM * identity + CUBIC_TERM * a + QUINTIC_TERM * s for a, s in zip(current, square)
        ]
        if counter + 1 < ITERS:
            halfway = [precise_dot(m, a) for m, a in zip(mixing, current)]
            current = [precise_dot(h, m) for h, m in zip(halfway, mixing)]
        total = mixing if total is None else [precise_dot(t, m) for t, m in zip(total, mixing)]
    scale = 0.2 * math.sqrt(depth)
    store_packed(out_ref, [t * (scale / b) for t, b in zip(total, bounds)])


def newton_schulz(estimate, gram, depth):
    per, width = gram.shape[:2]
    return pl.pallas_call(
        functools.partial(newton_schulz_kernel, depth),
        name="newton_schulz",
        out_shape=jax.ShapeDtypeStruct((packed_rows(per, width), width), F32),
    )(estimate, gram)


def apply_kernel(group_ref, factor_ref, *refs):
    del group_ref
    out_ref = refs[-1]
    per, _, width = out_ref.shape
    for i, factor in enumerate(unpack(factor_ref[0], per)):
        high, low = split(factor)
        right = jnp.concatenate(
            [
                jnp.concatenate([high, low], axis=1),
                jnp.concatenate([high, jnp.zeros_like(low)], axis=1),
            ],
            axis=0,
        )
        product = jnp.dot(refs[i][0], right, preferred_element_type=F32)
        out_ref[i] = product[:, :width] + product[:, width:]


def apply_factors(groups, factors, halves, per, partly=None):
    heads, rows, double = halves.shape
    width = double // 2
    count, packed = factors.shape[:2]
    by_group = lambda j, ids: (ids[j], 0, 0)
    operands = [groups, factors] + [halves] * per
    in_specs = [
        pl.BlockSpec((1, packed, width), lambda j, ids: (j, 0, 0)),
        *head_specs(per, (rows, double)),
    ]
    aliases = {}
    if partly is not None:
        operands.append(partly)
        in_specs.append(pl.BlockSpec(memory_space=pl.ANY))
        aliases = {2 + per: 0}
    return pl.pallas_call(
        apply_kernel,
        name="apply_factors",
        out_shape=jax.ShapeDtypeStruct((heads, rows, width), F32),
        grid_spec=pltpu.PrefetchScalarGridSpec(
            num_scalar_prefetch=1,
            grid=(count,),
            in_specs=in_specs,
            out_specs=pl.BlockSpec((per, rows, width), by_group),
        ),
        input_output_aliases=aliases,
        cost_estimate=pl.CostEstimate(
            flops=count * per * rows * width * width * 8,
            bytes_accessed=count * per * rows * width * 8,
            transcendentals=0,
        ),
        compiler_params=pltpu.CompilerParams(vmem_limit_bytes=ROOMY),
    )(*operands)


def swap(value, distance, devices):
    return lax.ppermute(value, "col", [(i, i ^ distance) for i in range(devices)])


def on_device(gradient, momentum, probe_vector, devices, axis_sizes):
    shape = gradient.shape
    heads, rows, width = shape[2:]
    gradient = gradient.reshape(heads, rows, width)
    momentum = momentum.reshape(heads, rows, width)
    chips = devices // 2
    per = heads // devices
    place = lax.axis_index("col")
    mine = jnp.stack([place ^ (2 * k) for k in range(chips)]).astype(jnp.int32)
    theirs = mine ^ 1
    groups = heads // per
    early = groups - groups // 3
    for_sibling = local_grams(theirs, gradient, momentum, per)
    from_sibling = swap(for_sibling, 1, devices)
    sums = local_grams(mine, gradient, momentum, per, from_sibling)
    pieces = [sums[0]]
    for k in range(1, chips):
        pieces.append(swap(sums[k], 2 * k, devices))
    gradient, momentum, anchor = lax.optimization_barrier((gradient, momentum, sums[0]))
    pieces[0] = anchor
    partly = update_momentum(gradient, momentum, per, 0, early)
    gram, estimate = sum_and_estimate(pieces, probe_vector.reshape(1, width), per)
    for name, size in axis_sizes:
        others = [
            lax.ppermute(estimate, name, [(i, (i + k) % size) for i in range(size)]) for k in range(1, size)
        ]
        for other in others:
            estimate = jnp.maximum(estimate, other)
    factor = newton_schulz(estimate, gram, rows * devices)
    factors = [factor]
    for k in range(1, chips):
        factors.append(swap(factor, 2 * k, devices))
    gradient, momentum, *partly = lax.optimization_barrier((gradient, momentum, *partly))
    new_momentum, halves = update_momentum(gradient, momentum, per, early, groups, partly)
    factors = jnp.stack(factors)
    sibling_factors = swap(factors, 1, devices)
    update = apply_factors(mine, factors, halves, per)
    update = apply_factors(theirs, sibling_factors, halves, per, update)
    return new_momentum.reshape(shape), update.reshape(shape)


def solution(mesh):
    sizes = dict(mesh.shape)
    devices = sizes["col"]
    axis_sizes = (("grp", sizes["grp"]), ("lay", sizes["lay"]))

    def body(gradient, momentum, probe_vector):
        groups, layers, heads = gradient.shape[:3]
        if groups == 1 and layers == 1 and heads % devices == 0 and devices > 1 and devices & (devices - 1) == 0:
            return on_device(gradient, momentum, probe_vector, devices, axis_sizes)
        return on_device_general(gradient, momentum, probe_vector)

    in_specs = (P("grp", "lay", None, "col", None), P("grp", "lay", None, "col", None), P())
    out_specs = (P("grp", "lay", None, "col", None), P("grp", "lay", None, "col", None))
    return jax.shard_map(
        body, mesh=mesh, in_specs=in_specs, out_specs=out_specs, check_vma=False
    )
```

```python
import functools
import math

import jax
import jax.numpy as jnp
from jax import lax
from jax.experimental import pallas as pl
from jax.experimental.pallas import tpu as pltpu
from jax.sharding import PartitionSpec as P


ITERS = 3


MOMENTUM_DECAY = 0.95
LINEAR_TERM = 3.4445
CUBIC_TERM = -4.775
QUINTIC_TERM = 2.0315
EPSILON = 1e-06
PRECISE = lax.Precision.HIGHEST


def summed_gram(stack):
    partial_gram = jnp.einsum("glhdr,glhds->glhrs", stack, stack, precision=PRECISE)
    return lax.psum(partial_gram, "col")


def head_bound(product, probe_norm):
    estimate = jnp.sqrt(jnp.sum(product * product, axis=-1) + EPSILON) / probe_norm
    local_most = jnp.max(estimate, axis=(0, 1))
    overall = lax.pmax(local_most, ("grp", "lay"))
    return 2.0 * jnp.sqrt(overall)


def on_device_general(gradient, momentum, probe_vector):
    new_momentum = MOMENTUM_DECAY * momentum + gradient
    blend = gradient + MOMENTUM_DECAY * new_momentum
    width = blend.shape[-1]
    probe_norm = jnp.sqrt(jnp.sum(probe_vector * probe_vector) + EPSILON)
    raw_gram = summed_gram(blend)
    product = jnp.einsum("glhrs,s->glhr", raw_gram, probe_vector, precision=PRECISE)
    bound_value = head_bound(product, probe_norm)
    scaled = blend / bound_value[None, None, :, None, None]
    current = raw_gram / (bound_value * bound_value)[None, None, :, None, None]
    identity = jnp.eye(width, dtype=jnp.float32)
    total = jnp.broadcast_to(identity, current.shape)
    for counter in range(ITERS):
        square = jnp.einsum("glhrs,glhst->glhrt", current, current, precision=PRECISE)
        mixing = LINEAR_TERM * identity + CUBIC_TERM * current + QUINTIC_TERM * square
        total = jnp.einsum("glhrs,glhst->glhrt", total, mixing, precision=PRECISE)
        if counter + 1 < ITERS:
            halfway = jnp.einsum("glhrs,glhst->glhrt", mixing, current, precision=PRECISE)
            current = jnp.einsum("glhrs,glhst->glhrt", halfway, mixing, precision=PRECISE)
    polished = jnp.einsum("glhdr,glhrs->glhds", scaled, total, precision=PRECISE)
    update = polished * (0.2 * math.sqrt(blend.shape[3] * lax.psum(1, "col")))
    return (new_momentum, update)


F32 = jnp.float32
BF16 = jnp.bfloat16
VMEM_LIMIT = 60 * 2**20
ROOMY = 48 * 2**20


def iotas(shape):
    return lax.broadcasted_iota(jnp.int32, shape, 0), lax.broadcasted_iota(jnp.int32, shape, 1)


def packed_rows(heads, width):
    full, odd = divmod(heads, 2)
    return full * width + odd * (width // 2) + 8 * (full + odd)


def pack(mats):
    width = mats[0].shape[0]
    row, col = iotas((width, width))
    rows8, _ = iotas((8, width))
    body, diags = [], []
    for i in range(0, len(mats) - 1, 2):
        first, second = mats[i], mats[i + 1]
        body.append(jnp.where(row >= col, first, second))
        diag = jnp.sum(jnp.where(row == col, second, 0.0), axis=0, keepdims=True)
        diags.append(jnp.where(rows8 == 0, diag, 0.0))
    if len(mats) % 2:
        half = width // 2
        last = mats[-1]
        row, col = iotas((half, width))
        rolled = pltpu.roll(last[half:], half, 1)
        body.append(jnp.where((col < half) & (col > row), rolled, last[:half]))
        diag = jnp.sum(jnp.where(row == col, rolled, 0.0), axis=0, keepdims=True)
        diags.append(jnp.where(rows8 == 0, diag, 0.0))
    return body + diags


def store_packed(ref, mats):
    start = 0
    for piece in pack(mats):
        ref[start : start + piece.shape[0]] = piece
        start += piece.shape[0]


def unpack(value, heads):
    width = value.shape[1]
    half = width // 2
    full, odd = divmod(heads, 2)
    diag_start = full * width + odd * half
    row, col = iotas((width, width))
    mats = []
    for i in range(full):
        square = value[i * width : (i + 1) * width]
        turned = square.T
        diag = value[diag_start + 8 * i : diag_start + 8 * i + 1]
        mats.append(jnp.where(row >= col, square, turned))
        mats.append(jnp.where(row < col, square, jnp.where(row > col, turned, diag)))
    if odd:
        top = value[full * width : full * width + half]
        turned = jnp.concatenate([top, jnp.zeros_like(top)], axis=0).T
        diag = value[diag_start + 8 * full : diag_start + 8 * full + 1]
        row, col = iotas((half, width))
        upper = jnp.where((col < half) & (row < col), turned[:half], top)
        corner = jnp.where(row < col, top, jnp.where(row > col, turned[:half], diag))
        lower = jnp.where(col < half, turned[half:], pltpu.roll(corner, half, 1))
        mats.append(jnp.concatenate([upper, lower], axis=0))
    return mats


def split(value):
    high = value.astype(BF16)
    return high, (value - high.astype(F32)).astype(BF16)


def head_specs(per, shape):
    return [pl.BlockSpec((1,) + shape, lambda j, ids, i=i: (ids[j] * per + i, 0, 0)) for i in range(per)]


def gram_kernel(per, group_ref, *refs):
    del group_ref
    gradient_refs, momentum_refs, refs = refs[:per], refs[per : 2 * per], refs[2 * per :]
    mats = []
    for gradient_ref, momentum_ref in zip(gradient_refs, momentum_refs):
        gradient = gradient_ref[0]
        blend = gradient + MOMENTUM_DECAY * (MOMENTUM_DECAY * momentum_ref[0] + gradient)
        high, low = split(blend)
        both = jnp.concatenate([high, low], axis=1)
        product = lax.dot_general(high, both, (((0,), (0,)), ((), ())), preferred_element_type=F32)
        width = blend.shape[1]
        cross = product[:, width:]
        mats.append(product[:, :width] + (cross + cross.T))
    if len(refs) == 1:
        store_packed(refs[0].at[0], mats)
        return
    other_ref, *out_refs, held_ref = refs
    store_packed(held_ref, mats)
    for k, out_ref in enumerate(out_refs):

        @pl.when(pl.program_id(0) == k)
        def _(out_ref=out_ref):
            out_ref[...] = held_ref[...] + other_ref[0]


def local_grams(groups, gradient, momentum, per, other=None):
    _, rows, width = gradient.shape
    count = groups.shape[0]
    blocks = head_specs(per, (rows, width))
    packed = packed_rows(per, width)
    piece = pl.BlockSpec((1, packed, width), lambda j, ids: (j, 0, 0))
    operands, in_specs = [groups] + [gradient] * per + [momentum] * per, blocks + blocks
    if other is None:
        out_shape = jax.ShapeDtypeStruct((count, packed, width), F32)
        out_specs, scratch = piece, []
    else:
        operands.append(other)
        in_specs.append(piece)
        out_shape = [jax.ShapeDtypeStruct((packed, width), F32)] * count
        out_specs = [pl.BlockSpec((packed, width), lambda j, ids: (0, 0))] * count
        scratch = [pltpu.VMEM((packed, width), F32)]
    return pl.pallas_call(
        functools.partial(gram_kernel, per),
        name="local_grams",
        out_shape=out_shape,
        grid_spec=pltpu.PrefetchScalarGridSpec(
            num_scalar_prefetch=1,
            grid=(count,),
            in_specs=in_specs,
            out_specs=out_specs,
            scratch_shapes=scratch,
        ),
        cost_estimate=pl.CostEstimate(
            flops=count * per * rows * width * width * 8,
            bytes_accessed=count * per * rows * width * 8,
            transcendentals=0,
        ),
        compiler_params=pltpu.CompilerParams(vmem_limit_bytes=VMEM_LIMIT),
    )(*operands)


def momentum_kernel(per, *refs):
    new_ref, halves_ref = refs[-2:]
    for i in range(per):
        gradient = refs[i][0]
        new = MOMENTUM_DECAY * refs[per + i][0] + gradient
        new_ref[i] = new
        high, low = split(gradient + MOMENTUM_DECAY * new)
        width = gradient.shape[1]
        halves_ref[i, :, :width] = high
        halves_ref[i, :, width:] = low


def update_momentum(gradient, momentum, per, start, stop, partly=()):
    heads, rows, width = gradient.shape
    by_group = lambda j: (j + start, 0, 0)
    block = pl.BlockSpec((per, rows, width), by_group)
    heads_of = [pl.BlockSpec((1, rows, width), lambda j, i=i: ((j + start) * per + i, 0, 0)) for i in range(per)]
    return pl.pallas_call(
        functools.partial(momentum_kernel, per),
        name="update_momentum",
        grid=(stop - start,),
        in_specs=heads_of + heads_of + [pl.BlockSpec(memory_space=pl.ANY)] * len(partly),
        out_specs=[block, pl.BlockSpec((per, rows, 2 * width), by_group)],
        out_shape=[
            jax.ShapeDtypeStruct(gradient.shape, F32),
            jax.ShapeDtypeStruct((heads, rows, 2 * width), BF16),
        ],
        input_output_aliases={2 * per: 0, 2 * per + 1: 1} if partly else {},
        cost_estimate=pl.CostEstimate(
            flops=(stop - start) * per * rows * width * 400,
            bytes_accessed=(stop - start) * per * rows * width * 16,
            transcendentals=0,
        ),
        compiler_params=pltpu.CompilerParams(vmem_limit_bytes=ROOMY),
    )(*[gradient] * per, *[momentum] * per, *partly)


def estimate_kernel(per, probe_ref, *refs):
    *pieces, gram_ref, estimate_ref = refs
    total = pieces[0][...]
    for piece in pieces[1:]:
        total = total + piece[...]
    probe = probe_ref[...]
    probe_norm = jnp.sqrt(jnp.sum(probe * probe, keepdims=True) + EPSILON)
    row, _ = iotas(estimate_ref.shape)
    estimates = jnp.zeros(estimate_ref.shape, F32)
    for i, gram in enumerate(unpack(total, per)):
        gram_ref[i] = gram
        product = jnp.sum(gram * probe, axis=1, keepdims=True)
        estimate = jnp.sqrt(jnp.sum(product * product, keepdims=True) + EPSILON) / probe_norm
        estimates = jnp.where(row == i, estimate, estimates)
    estimate_ref[...] = estimates


def sum_and_estimate(pieces, probe, per):
    width = pieces[0].shape[1]
    return pl.pallas_call(
        functools.partial(estimate_kernel, per),
        name="sum_and_estimate",
        out_shape=[
            jax.ShapeDtypeStruct((per, width, width), F32),
            jax.ShapeDtypeStruct((-(-per // 8) * 8, width), F32),
        ],
    )(probe, *pieces)


def precise_dot(left, right):
    return jnp.dot(left, right, precision=PRECISE, preferred_element_type=F32)


def newton_schulz_kernel(depth, estimate_ref, gram_ref, out_ref):
    per, width = gram_ref.shape[:2]
    row, col = iotas((width, width))
    identity = jnp.where(row == col, 1.0, 0.0)
    bounds = [2.0 * jnp.sqrt(estimate_ref[i : i + 1]) for i in range(per)]
    current = [gram_ref[i] / (bounds[i] * bounds[i]) for i in range(per)]
    total = None
    for counter in range(ITERS):
        square = [precise_dot(a, a) for a in current]
        mixing = [
            LINEAR_TERM * identity + CUBIC_TERM * a + QUINTIC_TERM * s for a, s in zip(current, square)
        ]
        if counter + 1 < ITERS:
            halfway = [precise_dot(m, a) for m, a in zip(mixing, current)]
            current = [precise_dot(h, m) for h, m in zip(halfway, mixing)]
        total = mixing if total is None else [precise_dot(t, m) for t, m in zip(total, mixing)]
    scale = 0.2 * math.sqrt(depth)
    store_packed(out_ref, [t * (scale / b) for t, b in zip(total, bounds)])


def newton_schulz(estimate, gram, depth):
    per, width = gram.shape[:2]
    return pl.pallas_call(
        functools.partial(newton_schulz_kernel, depth),
        name="newton_schulz",
        out_shape=jax.ShapeDtypeStruct((packed_rows(per, width), width), F32),
    )(estimate, gram)


def apply_kernel(group_ref, factor_ref, *refs):
    del group_ref
    out_ref = refs[-1]
    per, _, width = out_ref.shape
    for i, factor in enumerate(unpack(factor_ref[0], per)):
        high, low = split(factor)
        right = jnp.concatenate(
            [
                jnp.concatenate([high, low], axis=1),
                jnp.concatenate([high, jnp.zeros_like(low)], axis=1),
            ],
            axis=0,
        )
        product = jnp.dot(refs[i][0], right, preferred_element_type=F32)
        out_ref[i] = product[:, :width] + product[:, width:]


def apply_factors(groups, factors, halves, per, partly=None):
    heads, rows, double = halves.shape
    width = double // 2
    count, packed = factors.shape[:2]
    by_group = lambda j, ids: (ids[j], 0, 0)
    operands = [groups, factors] + [halves] * per
    in_specs = [
        pl.BlockSpec((1, packed, width), lambda j, ids: (j, 0, 0)),
        *head_specs(per, (rows, double)),
    ]
    aliases = {}
    if partly is not None:
        operands.append(partly)
        in_specs.append(pl.BlockSpec(memory_space=pl.ANY))
        aliases = {2 + per: 0}
    return pl.pallas_call(
        apply_kernel,
        name="apply_factors",
        out_shape=jax.ShapeDtypeStruct((heads, rows, width), F32),
        grid_spec=pltpu.PrefetchScalarGridSpec(
            num_scalar_prefetch=1,
            grid=(count,),
            in_specs=in_specs,
            out_specs=pl.BlockSpec((per, rows, width), by_group),
        ),
        input_output_aliases=aliases,
        cost_estimate=pl.CostEstimate(
            flops=count * per * rows * width * width * 8,
            bytes_accessed=count * per * rows * width * 8,
            transcendentals=0,
        ),
        compiler_params=pltpu.CompilerParams(vmem_limit_bytes=ROOMY),
    )(*operands)


def swap(value, distance, devices):
    return lax.ppermute(value, "col", [(i, i ^ distance) for i in range(devices)])


def on_device(gradient, momentum, probe_vector, devices, axis_sizes):
    shape = gradient.shape
    heads, rows, width = shape[2:]
    gradient = gradient.reshape(heads, rows, width)
    momentum = momentum.reshape(heads, rows, width)
    chips = devices // 2
    per = heads // devices
    place = lax.axis_index("col")
    mine = jnp.stack([place ^ (2 * k) for k in range(chips)]).astype(jnp.int32)
    theirs = mine ^ 1
    groups = heads // per
    late = groups - groups // 4
    begun = late - len(axis_sizes)
    for_sibling = local_grams(theirs, gradient, momentum, per)
    from_sibling = swap(for_sibling, 1, devices)
    sums = local_grams(mine, gradient, momentum, per, from_sibling)
    pieces = [sums[0]]
    for k in range(1, chips):
        pieces.append(swap(sums[k], 2 * k, devices))
    gradient, momentum, anchor = lax.optimization_barrier((gradient, momentum, sums[0]))
    pieces[0] = anchor
    partly = update_momentum(gradient, momentum, per, 0, begun)
    gram, estimate = sum_and_estimate(pieces, probe_vector.reshape(1, width), per)
    for name, size in axis_sizes:
        others = []
        for k in range(1, size):
            others.append(lax.ppermute(estimate, name, [(i, (i + k) % size) for i in range(size)]))
        partly = update_momentum(gradient, momentum, per, begun, begun + 1, partly)
        begun += 1
        for other in others:
            estimate = jnp.maximum(estimate, other)
    factor = newton_schulz(estimate, gram, rows * devices)
    factors = [factor]
    for k in range(1, chips):
        factors.append(swap(factor, 2 * k, devices))
    gradient, momentum, *partly = lax.optimization_barrier((gradient, momentum, *partly))
    new_momentum, halves = update_momentum(gradient, momentum, per, late, groups, partly)
    factors = jnp.stack(factors)
    sibling_factors = swap(factors, 1, devices)
    update = apply_factors(mine, factors, halves, per)
    update = apply_factors(theirs, sibling_factors, halves, per, update)
    return new_momentum.reshape(shape), update.reshape(shape)


def solution(mesh):
    sizes = dict(mesh.shape)
    devices = sizes["col"]
    axis_sizes = (("grp", sizes["grp"]), ("lay", sizes["lay"]))

    def body(gradient, momentum, probe_vector):
        groups, layers, heads = gradient.shape[:3]
        if groups == 1 and layers == 1 and heads % devices == 0 and devices > 4 and devices & (devices - 1) == 0:
            return on_device(gradient, momentum, probe_vector, devices, axis_sizes)
        return on_device_general(gradient, momentum, probe_vector)

    in_specs = (P("grp", "lay", None, "col", None), P("grp", "lay", None, "col", None), P())
    out_specs = (P("grp", "lay", None, "col", None), P("grp", "lay", None, "col", None))
    return jax.shard_map(
        body, mesh=mesh, in_specs=in_specs, out_specs=out_specs, check_vma=False
    )
```
